32 devices in a mesh: dp: 4 (over x, y), sp: 8 (over z, core).
Axes of the slice: x: 2, y: 2, z: 4, core: 2. Of those that a mesh axis runs over, the one named last changes fastest.
Arguments:
- q: bfloat16 [128, 24, 128], P('dp'), parts along dimension 0
- k: bfloat16 [128, 8192, 8, 128], P('dp', 'sp'), parts along dimension 0
- v: bfloat16 [128, 8192, 8, 128], P('dp', 'sp'), parts along dimension 0
Outputs:
- q: bfloat16 [128, 24, 128], P('dp'), parts along dimension 0
There are 4 independent parts. The reference program is written for one: setup_inputs(seed, part) draws one part's arguments, and reference() takes and returns one part's arrays. A program takes and returns all parts, laid end to end along the dimension named above; each array names one.
All inputs are finite; a program needn't handle non-finite values.
Results may differ from the reference program's by a relative error of at most 0.012.
Values are sent between devices in bfloat16 or wider.
A program may use at most 2 GiB of HBM per device.

```python
import jax
import jax.numpy as jnp

BATCH = 32
CACHE = 8192
HEADS = 24
KV_HEADS = 8
HEAD = 128


def setup_inputs(seed: int = 0, part: int = 0) -> dict:
    kq, kk, kv = (jax.random.fold_in(k, part) for k in jax.random.split(jax.random.key(seed), 3))
    return {
        "q": (3 * jax.random.normal(kq, (BATCH, HEADS, HEAD), jnp.float32)).astype(jnp.bfloat16),
        "k": jax.random.normal(kk, (BATCH, CACHE, KV_HEADS, HEAD), jnp.float32).astype(jnp.bfloat16),
        "v": jax.random.normal(kv, (BATCH, CACHE, KV_HEADS, HEAD), jnp.float32).astype(jnp.bfloat16),
    }


def einsum(form, a, b):
    return jnp.einsum(form, a.astype(jnp.float32), b.astype(jnp.float32))


def reference(q, k, v):
    grouped = q.reshape(BATCH, KV_HEADS, -1, HEAD)
    scores = einsum("bgsd,bugd->bgsu", grouped, k) * HEAD**-0.5
    weights = jax.nn.softmax(scores, -1).astype(jnp.bfloat16)
    return einsum("bgsu,bugd->bgsd", weights, v).astype(jnp.bfloat16).reshape(BATCH, HEADS, HEAD)
```

```python
import functools
import math

import jax
import jax.numpy as jnp
from jax import lax
from jax.experimental import pallas as pl
from jax.experimental.pallas import tpu as pltpu
from jax.sharding import PartitionSpec as P

MESH = pl.DeviceIdType.MESH
LANES = 128
SLOTS = 6
LAG = 6
TAIL = 8


def kernel(n, kv_heads, q_ref, k_ref, v_ref, o_ref, k_buf, v_buf, s_buf, w_buf, m_buf, parts, stats, k_sem, v_sem, ps_sem, pr_sem, ss_sem, sr_sem, os_sem, or_sem):
    split = q_ref.shape[0] - TAIL
    batch, heads, head = q_ref.shape
    rows = k_ref.shape[1]
    half = rows // 2
    quarter = rows // 4
    blocks = half // LANES
    c = head**-0.5 * math.log2(math.e)
    me = lax.axis_index("sp")

    def k_copy(i):
        return pltpu.make_async_copy(k_ref.at[i], k_buf.at[lax.rem(i, SLOTS)], k_sem.at[lax.rem(i, SLOTS)])

    def v_copy(i, part):
        at = pl.ds(part * half, half)
        slot = lax.rem(i, SLOTS)
        return pltpu.make_async_copy(v_ref.at[i, at], v_buf.at[slot, at], v_sem.at[slot, part])

    row = lax.broadcasted_iota(jnp.int32, (heads, LANES), 0)
    lane = lax.broadcasted_iota(jnp.int32, (heads, LANES), 1)
    own = lax.rem(lane, kv_heads) == row // (heads // kv_heads)
    own = jnp.concatenate([own, own], 0)
    diagonal = row == lane

    def scores(i):
        q = q_ref[i].astype(jnp.float32)
        zero = jnp.zeros_like(q)
        both = jnp.concatenate([jnp.concatenate([q, zero], 1), jnp.concatenate([zero, q], 1)], 0).astype(jnp.bfloat16)
        slot = lax.rem(i, SLOTS)
        high = None
        for part in range(2):
            keys = jnp.concatenate(
                [k_buf[slot, pl.ds(part * quarter, quarter)], k_buf[slot, pl.ds(half + part * quarter, quarter)]], 1
            )
            s = lax.dot_general(both, keys, (((1,), (1,)), ((), ())), preferred_element_type=jnp.float32)
            for j in range(quarter // LANES):
                block = jnp.where(own, s[:, j * LANES : (j + 1) * LANES], -jnp.inf)
                s_buf[:, pl.ds(part * quarter + j * LANES, LANES)] = block
                high = block if high is None else jnp.maximum(high, block)
        m_buf[...] = jnp.maximum(high[:heads], high[heads:])

    def weigh():
        m = jnp.broadcast_to(jnp.max(m_buf[...], 1, keepdims=True), (heads, LANES))
        high = jnp.concatenate([m, m], 0)
        total = None
        for j in range(blocks):
            at = pl.ds(j * LANES, LANES)
            w = jnp.exp2((s_buf[:, at] - high) * c)
            total = w if total is None else total + w
            w_buf[:, at] = w.astype(jnp.bfloat16)
        return m, jnp.sum(total[:heads] + total[heads:], 1, keepdims=True)

    def attend(i, m, total):
        slot = lax.rem(i, SLOTS)
        seen = None
        for part in range(2):
            values = jnp.concatenate(
                [v_buf[slot, pl.ds(part * quarter, quarter)], v_buf[slot, pl.ds(half + part * quarter, quarter)]], 1
            )
            r = jnp.dot(w_buf[:, pl.ds(part * quarter, quarter)], values, preferred_element_type=jnp.float32)
            r = r[:heads, :head] + r[heads:, head:]
            seen = r if seen is None else seen + r
        parts[i, me] = seen.astype(jnp.bfloat16)
        m_row = jnp.sum(jnp.where(diagonal, m, 0.0), 0, keepdims=True)
        l_row = jnp.sum(jnp.where(diagonal, total, 0.0), 0, keepdims=True)
        stats[i, me] = jnp.concatenate([m_row, l_row], 1)

    def remote(ref, i, owner, peer, send_sem, recv_sem):
        return pltpu.make_async_remote_copy(
            ref.at[i, owner], ref.at[i, owner], send_sem.at[i], recv_sem.at[i], device_id={"sp": peer}, device_id_type=MESH
        )

    def send(i, peer):
        remote(stats, i, me, peer, ss_sem, sr_sem).start()
        remote(parts, i, me, peer, ps_sem, pr_sem).start()

    def arrived(ref, i, count, sem):
        at = ref.at[i, pl.ds(0, count)]
        pltpu.make_async_copy(at, at, sem.at[i]).wait()

    def sent(i, count):
        arrived(stats, i, count, ss_sem)
        arrived(parts, i, count, ps_sem)

    def peers(do):
        for t in range(1, n):
            do(lax.rem(me + t, n))

    def combine(i):
        arrived(stats, i, n - 1, sr_sem)
        arrived(parts, i, n - 1, pr_sem)
        m = stats[i, :, 0, pl.ds(0, LANES)]
        l = stats[i, :, 0, pl.ds(LANES, LANES)]
        w = jnp.exp2((m - jnp.max(m, 0, keepdims=True)) * c)
        factor = w / jnp.sum(w * l, 0, keepdims=True)
        columns = factor.T
        out = None
        for d in range(n):
            r = parts[i, d].astype(jnp.float32) * columns[:heads, d : d + 1]
            out = r if out is None else out + r
        o_ref[i] = out.astype(o_ref.dtype)

    def share(i, peer):
        return pltpu.make_async_remote_copy(
            o_ref.at[i], o_ref.at[i], os_sem.at[i], or_sem.at[i], device_id={"sp": peer}, device_id_type=MESH
        )

    def shared(i):
        at = o_ref.at[pl.ds(0, n - 1)]
        pltpu.make_async_copy(at, at, os_sem.at[i]).wait()

    def exchange(i):
        @pl.when(jnp.logical_and(i >= 2, jnp.logical_and(i - 2 < split, lax.rem(i - 2, n) != me)))
        def _():
            send(i - 2, lax.rem(i - 2, n))

        @pl.when(i - 2 >= split)
        def _():
            peers(lambda peer: send(i - 2, peer))

        j = i - LAG

        @pl.when(jnp.logical_and(j >= 0, j < split))
        def _():
            @pl.when(lax.rem(j, n) == me)
            def _():
                combine(j)

            @pl.when(lax.rem(j, n) != me)
            def _():
                sent(j, 1)

        @pl.when(jnp.logical_and(j >= 1, j - 1 < split))
        def _():
            @pl.when(lax.rem(j - 1, n) == me)
            def _():
                peers(lambda peer: share(j - 1, peer).start())

    k_copy(0).start()
    k_copy(1).start()
    for i in range(SLOTS - 2):
        for part in range(2):
            v_copy(i, part).start()
        k_copy(i + 2).start()
    for i in range(SLOTS - 2, SLOTS):
        for part in range(2):
            v_copy(i, part).start()

    barrier = pltpu.get_barrier_semaphore()
    for t in range(1, n):
        pl.semaphore_signal(barrier, inc=1, device_id={"sp": lax.rem(me + t, n)}, device_id_type=MESH)

    k_copy(0).wait()
    scores(0)

    @pl.when(SLOTS < batch)
    def _():
        k_copy(SLOTS).start()

    pl.semaphore_wait(barrier, n - 1)

    @pl.loop(1, batch)
    def _(i):
        exchange(i)
        k_copy(i).wait()
        for part in range(2):
            v_copy(i - 1, part).wait()
        m, total = weigh()
        scores(i)
        attend(i - 1, m, total)

        @pl.when(i + SLOTS < batch)
        def _():
            k_copy(i + SLOTS).start()

        @pl.when(i - 1 + SLOTS < batch)
        def _():
            for part in range(2):
                v_copy(i - 1 + SLOTS, part).start()

    peers(lambda peer: send(batch - 2, peer))
    m, total = weigh()
    for part in range(2):
        v_copy(batch - 1, part).wait()
    attend(batch - 1, m, total)
    peers(lambda peer: send(batch - 1, peer))

    @pl.loop(split, batch)
    def _(i):
        combine(i)
        sent(i, n - 1)

    @pl.loop(0, split)
    def _(i):
        @pl.when(lax.rem(i, n) == me)
        def _():
            shared(i)

        @pl.when(lax.rem(i, n) != me)
        def _():
            share(i, me).wait_recv()


def solution(mesh):
    n = mesh.shape["sp"]

    def step(q, k, v):
        batch, heads, head = q.shape
        tokens, kv_heads = k.shape[1:3]
        rows = tokens * kv_heads
        k, v = k.reshape(batch, rows, head), v.reshape(batch, rows, head)
        return pl.pallas_call(
            functools.partial(kernel, n, kv_heads),
            out_shape=jax.ShapeDtypeStruct(q.shape, q.dtype),
            in_specs=[
                pl.BlockSpec(memory_space=pltpu.VMEM),
                pl.BlockSpec(memory_space=pl.ANY),
                pl.BlockSpec(memory_space=pl.ANY),
            ],
            out_specs=pl.BlockSpec(memory_space=pltpu.VMEM),
            scratch_shapes=[
                pltpu.VMEM((SLOTS, rows, head), jnp.bfloat16),
                pltpu.VMEM((SLOTS, rows, head), jnp.bfloat16),
                pltpu.VMEM((2 * heads, rows // 2), jnp.float32),
                pltpu.VMEM((2 * heads, rows // 2), jnp.bfloat16),
                pltpu.VMEM((heads, LANES), jnp.float32),
                pltpu.VMEM((batch, n, heads, head), jnp.bfloat16),
                pltpu.VMEM((batch, n, 1, 2 * LANES), jnp.float32),
                pltpu.SemaphoreType.DMA((SLOTS,)),
                pltpu.SemaphoreType.DMA((SLOTS, 2)),
                pltpu.SemaphoreType.DMA((batch,)),
                pltpu.SemaphoreType.DMA((batch,)),
                pltpu.SemaphoreType.DMA((batch,)),
                pltpu.SemaphoreType.DMA((batch,)),
                pltpu.SemaphoreType.DMA((batch,)),
                pltpu.SemaphoreType.DMA((batch,)),
            ],
            compiler_params=pltpu.CompilerParams(collective_id=0, has_side_effects=True, vmem_limit_bytes=60 * 2**20),
        )(q, k, v)

    return jax.shard_map(
        step,
        mesh=mesh,
        in_specs=(P("dp", None, None), P("dp", "sp", None, None), P("dp", "sp", None, None)),
        out_specs=P("dp", None, None),
        check_vma=False,
    )
```

```python
import functools
import math

import jax
import jax.numpy as jnp
from jax import lax
from jax.experimental import pallas as pl
from jax.experimental.pallas import tpu as pltpu
from jax.sharding import PartitionSpec as P

MESH = pl.DeviceIdType.MESH
LANES = 128
SLOTS = 6
TAIL = 4
LAG = 2


def kernel(
    n, kv_heads, q_hbm, k_ref, v_ref, o_ref, q_ref, k_buf, v_buf, s_buf, w_buf, m_buf, parts, stats,
    q_sem, k_sem, v_sem, ps_sem, pr_sem, ss_sem, sr_sem, os_sem, or_sem,
):
    batch, heads, head = q_ref.shape
    rows = k_ref.shape[1]
    half = rows // 2
    quarter = rows // 4
    pairs = batch // 2
    split = pairs - TAIL
    c = head**-0.5 * math.log2(math.e)
    me = lax.axis_index("sp")

    def q_copy():
        return pltpu.make_async_copy(q_hbm, q_ref, q_sem)

    def k_copy(i):
        return pltpu.make_async_copy(k_ref.at[i], k_buf.at[lax.rem(i, SLOTS)], k_sem.at[lax.rem(i, SLOTS)])

    def v_copy(i, part):
        at = pl.ds(part * half, half)
        slot = lax.rem(i, SLOTS)
        return pltpu.make_async_copy(v_ref.at[i, at], v_buf.at[slot, at], v_sem.at[slot, part])

    def v_start(i):
        for part in range(2):
            v_copy(i, part).start()

    def v_wait(i):
        for part in range(2):
            v_copy(i, part).wait()

    row = lax.broadcasted_iota(jnp.int32, (heads, LANES), 0)
    lane = lax.broadcasted_iota(jnp.int32, (heads, LANES), 1)
    own = lax.rem(lane, kv_heads) == row // (heads // kv_heads)
    own = jnp.concatenate([own, own], 0)
    diagonal = row == lane

    def side_by_side(buf, slot, part):
        return jnp.concatenate([buf[slot, pl.ds(part * half, quarter)], buf[slot, pl.ds(part * half + quarter, quarter)]], 1)

    def scores(i):
        q = q_ref[i].astype(jnp.float32)
        zero = jnp.zeros_like(q)
        both = jnp.concatenate([jnp.concatenate([q, zero], 1), jnp.concatenate([zero, q], 1)], 0).astype(jnp.bfloat16)
        high = None
        for part in range(2):
            keys = side_by_side(k_buf, lax.rem(i, SLOTS), part)
            s = lax.dot_general(both, keys, (((1,), (1,)), ((), ())), preferred_element_type=jnp.float32)
            for j in range(quarter // LANES):
                block = jnp.where(own, s[:, j * LANES : (j + 1) * LANES], -jnp.inf)
                s_buf[:, pl.ds(part * quarter + j * LANES, LANES)] = block
                high = block if high is None else jnp.maximum(high, block)
        m_buf[...] = jnp.maximum(high[:heads], high[heads:])

    def weigh(turn):
        m = jnp.broadcast_to(jnp.max(m_buf[...], 1, keepdims=True), (heads, LANES))
        high = jnp.concatenate([m, m], 0)
        total = None
        for j in range(half // LANES):
            at = pl.ds(j * LANES, LANES)
            w = jnp.exp2((s_buf[:, at] - high) * c)
            total = w if total is None else total + w
            w_buf[turn, :, at] = w.astype(jnp.bfloat16)
        return m, jnp.sum(total[:heads] + total[heads:], 1, keepdims=True)

    def keep(i, m, total):
        m_row = jnp.sum(jnp.where(diagonal, m, 0.0), 0, keepdims=True)
        l_row = jnp.sum(jnp.where(diagonal, total, 0.0), 0, keepdims=True)
        stats[i, me] = jnp.concatenate([m_row, l_row], 1)

    def attend(i, turn, part):
        values = side_by_side(v_buf, lax.rem(i, SLOTS), part)
        r = jnp.dot(w_buf[turn, :, pl.ds(part * quarter, quarter)], values, preferred_element_type=jnp.float32)
        return r[:heads, :head] + r[heads:, head:]

    def attend_all(i, turn):
        parts[i, me] = (attend(i, turn, 0) + attend(i, turn, 1)).astype(jnp.bfloat16)

    def remote(ref, first, count, p, peer, send_sem, recv_sem):
        at = ref.at[pl.ds(first, count), me]
        return pltpu.make_async_remote_copy(at, at, send_sem.at[p], recv_sem.at[p], device_id={"sp": peer}, device_id_type=MESH)

    def send(first, count, p, peer):
        remote(stats, first, count, p, peer, ss_sem, sr_sem).start()
        remote(parts, first, count, p, peer, ps_sem, pr_sem).start()

    def peers(do):
        upper = me >= n // 2
        mine = jnp.where(upper, me, n - 1 - me)
        for t in range(n - 1):
            d = jnp.where(t >= mine, t + 1, t)
            do(jnp.where(upper, d, n - 1 - d))

    def finish(ref, first, count, times, sem):
        at = ref.at[pl.ds(first, count), pl.ds(0, times)]
        pltpu.make_async_copy(at, at, sem).wait()

    def sent(first, count, p, times):
        finish(stats, first, count, times, ss_sem.at[p])
        finish(parts, first, count, times, ps_sem.at[p])

    def combine(first, count, p):
        finish(stats, first, count, n - 1, sr_sem.at[p])
        finish(parts, first, count, n - 1, pr_sem.at[p])
        for i in range(count):
            i = first + i
            m = stats[i, :, 0, pl.ds(0, LANES)]
            l = stats[i, :, 0, pl.ds(LANES, LANES)]
            w = jnp.exp2((m - jnp.max(m, 0, keepdims=True)) * c)
            columns = (w / jnp.sum(w * l, 0, keepdims=True)).T
            out = None
            for d in range(n):
                r = parts[i, d].astype(jnp.float32) * columns[:heads, d : d + 1]
                out = r if out is None else out + r
            o_ref[i] = out.astype(o_ref.dtype)

    def share(p, peer):
        at = o_ref.at[pl.ds(2 * p, 2)]
        return pltpu.make_async_remote_copy(at, at, os_sem.at[p], or_sem.at[p], device_id={"sp": peer}, device_id_type=MESH)

    def share_all(p):
        @pl.when(jnp.logical_and(jnp.logical_and(p >= 0, p < split), lax.rem(p, n) == me))
        def _():
            peers(lambda peer: share(p, peer).start())

    def exchange(p):
        owner = lax.rem(jnp.maximum(p, 0), n)

        @pl.when(jnp.logical_and(jnp.logical_and(p >= 0, p < split), owner != me))
        def _():
            send(2 * p, 2, p, owner)

        @pl.when(p >= split)
        def _():
            peers(lambda peer: send(2 * p, 2, p, peer))

        share_all(p - LAG - 1)
        ready = p - LAG

        @pl.when(jnp.logical_and(jnp.logical_and(ready >= 0, ready < split), lax.rem(jnp.maximum(ready, 0), n) == me))
        def _():
            combine(2 * ready, 2, ready)

    k_copy(0).start()
    q_copy().start()
    k_copy(1).start()
    v_start(0)
    k_copy(2).start()
    v_start(1)

    barrier = pltpu.get_barrier_semaphore()
    for t in range(1, n):
        pl.semaphore_signal(barrier, inc=1, device_id={"sp": lax.rem(me + t, n)}, device_id_type=MESH)

    q_copy().wait()
    k_copy(0).wait()
    for i in range(2, SLOTS - 2):
        k_copy(i + 1).start()
        v_start(i)
    scores(0)
    for i in range(SLOTS - 2, SLOTS):
        k_copy(i + 1).start()
        v_start(i)
    pl.semaphore_wait(barrier, n - 1)

    @pl.loop(0, pairs - 1)
    def _(p):
        i = 2 * p + 1
        exchange(p - 1)
        for t in range(2):
            k_copy(i + t).wait()
            v_wait(i - 1 + t)
        for t in range(2):
            m, total = weigh(t)
            scores(i + t)
            attend_all(i - 1 + t, t)
            keep(i - 1 + t, m, total)

        for t in range(2):

            @pl.when(i + t + SLOTS < batch)
            def _():
                k_copy(i + t + SLOTS).start()

            @pl.when(i - 1 + t + SLOTS < batch)
            def _():
                v_start(i - 1 + t + SLOTS)

    last = batch - 1
    exchange(jnp.int32(pairs - 2))
    k_copy(last).wait()
    m, total = weigh(0)
    scores(last)
    keep(last - 1, m, total)
    v_wait(last - 1)
    m, total = weigh(1)
    attend_all(last - 1, 0)
    keep(last, m, total)
    peers(lambda peer: send(last - 1, 1, pairs - 1, peer))
    v_copy(last, 0).wait()
    r = attend(last, 1, 0)
    v_copy(last, 1).wait()
    parts[last, me] = (r + attend(last, 1, 1)).astype(jnp.bfloat16)
    peers(lambda peer: send(last, 1, pairs, peer))

    @pl.loop(split, pairs - 1)
    def _(p):
        combine(2 * p, 2, p)
        sent(2 * p, 2, p, n - 1)

    @pl.loop(0, split)
    def _(p):
        @pl.when(lax.rem(p, n) == me)
        def _():
            at = o_ref.at[pl.ds(0, 2 * (n - 1))]
            pltpu.make_async_copy(at, at, os_sem.at[p]).wait()

        @pl.when(lax.rem(p, n) != me)
        def _():
            sent(2 * p, 2, p, 1)
            share(p, me).wait_recv()

    combine(last - 1, 1, pairs - 1)
    sent(last - 1, 1, pairs - 1, n - 1)
    sent(last, 1, pairs, n - 1)
    combine(last, 1, pairs)


def solution(mesh):
    n = mesh.shape["sp"]

    def step(q, k, v):
        batch, heads, head = q.shape
        tokens, kv_heads = k.shape[1:3]
        rows = tokens * kv_heads
        k, v = k.reshape(batch, rows, head), v.reshape(batch, rows, head)
        return pl.pallas_call(
            functools.partial(kernel, n, kv_heads),
            out_shape=pltpu.VMEM(q.shape, q.dtype),
            in_specs=[pl.BlockSpec(memory_space=pl.ANY)] * 3,
            out_specs=pl.BlockSpec(memory_space=pltpu.VMEM),
            scratch_shapes=[
                pltpu.VMEM((batch, heads, head), jnp.bfloat16),
                pltpu.VMEM((SLOTS, rows, head), jnp.bfloat16),
                pltpu.VMEM((SLOTS, rows, head), jnp.bfloat16),
                pltpu.VMEM((2 * heads, rows // 2), jnp.float32),
                pltpu.VMEM((2, 2 * heads, rows // 2), jnp.bfloat16),
                pltpu.VMEM((heads, LANES), jnp.float32),
                pltpu.VMEM((batch, n, heads, head), jnp.bfloat16),
                pltpu.VMEM((batch, n, 1, 2 * LANES), jnp.float32),
                pltpu.SemaphoreType.DMA,
                pltpu.SemaphoreType.DMA((SLOTS,)),
                pltpu.SemaphoreType.DMA((SLOTS, 2)),
            ]
            + [pltpu.SemaphoreType.DMA((batch // 2 + 1,))] * 6,
            compiler_params=pltpu.CompilerParams(collective_id=0, has_side_effects=True, vmem_limit_bytes=56 * 2**20),
        )(q, k, v)

    return jax.shard_map(
        step,
        mesh=mesh,
        in_specs=(P("dp", None, None), P("dp", "sp", None, None), P("dp", "sp", None, None)),
        out_specs=P("dp", None, None),
        check_vma=False,
    )
```
